32 devices in a mesh: section: 2 (over core), dev: 16 (over z, y, x).
Axes of the slice: x: 2, y: 2, z: 4, core: 2. Of those that a mesh axis runs over, the one named last changes fastest.
Arguments:
- indices: int32 [2048, 32, 8], P(('section', 'dev')), may hold values from 0 to 32767
- pool_len: int32 [32], replicated, may hold values from 1 to 8
- tables: bfloat16 [1048576, 128], P(('section', 'dev')), may hold values from -3 to 3
- w_first: bfloat16 [4096, 4096], P('dev', 'section'), may hold values from -0.09375 to 0.09375
- b_first: bfloat16 [4096], P('section'), may hold values from -3 to 3
- w_out: bfloat16 [4096], P('section'), may hold values from -0.09375 to 0.09375
Outputs:
- logits: float32 [2048], P('dev')
The draws below stay inside these ranges and needn't reach their ends.
Inputs may be any that keep to these rules, and one draw needn't show every extreme that they name: `indices`: ids of rows of the table named by the second index.
All inputs are finite; a program needn't handle non-finite values.
Results may differ from the reference program's by a relative error of at most 0.0095.
Values may be sent and summed in bfloat16 or wider, within the bound.
A program may use at most 128 MiB of HBM per device.

```python
import jax
import jax.numpy as jnp
from jax import lax

E = 128
HID = 4096
TABLES = 32
POOL = 8
ROWS_DEV = 32768
RSPLIT = 1
ROWS = 32768
FEAT = 4096
BATCH = 2048


def plant(array, key, low, top_value):
    longest = array.shape.index(max(array.shape))
    spots = []
    for shift in (0, 1):
        where = [jax.random.randint(jax.random.fold_in(key, axis), (), 0, length) for axis, length in enumerate(array.shape)]
        where[longest] = (where[longest] + shift) % array.shape[longest]
        spots.append(tuple(where))
    return array.at[spots[0]].set(low).at[spots[1]].set(top_value)


def block_levels(key, shape, split, smallest, largest):
    level, own = 1.0, jax.random.fold_in(key, 6)
    for position, parts in split:
        draws = jnp.exp(jax.random.uniform(jax.random.fold_in(own, position), (parts,), jnp.float32, smallest / len(split), largest / len(split)))
        level = level * jnp.repeat(draws, shape[position] // parts).reshape([-1 if axis == position else 1 for axis in range(len(shape))])
    return level


def scatter_about(rng, dims, spread, limit, split=(), dtype=jnp.bfloat16):
    factor_of = block_levels(rng, dims, split, -0.22, 0.18) if split else 1.0
    values = jax.random.normal(rng, dims, jnp.float32) * spread * factor_of
    return jnp.minimum(jnp.maximum(values, -limit), limit).astype(dtype)


def setup_inputs(seed: int = 0) -> dict:
    arg_keys = jax.random.split(jax.random.key(seed), 7)
    indices = plant(jax.random.randint(arg_keys[0], (BATCH, TABLES, POOL), 0, ROWS), jax.random.fold_in(arg_keys[0], 1), 0, ROWS - 1).astype(jnp.int32)
    pool_len = plant(jax.random.randint(arg_keys[1], (TABLES,), 1, POOL + 1), jax.random.fold_in(arg_keys[1], 1), 1, POOL).astype(jnp.int32)
    tables = scatter_about(arg_keys[2], (TABLES * ROWS, E), 0.5, 3.0, ((0, 32),))
    w_first = scatter_about(arg_keys[3], (FEAT, HID), FEAT ** -0.5, 0.09375, ((0, 16), (1, 2)))
    b_first = scatter_about(arg_keys[4], (HID,), 0.5, 3.0, ((0, 2),))
    w_out = scatter_about(arg_keys[5], (HID,), HID ** -0.5, 0.09375, ((0, 2),))
    return {"indices": indices, "pool_len": pool_len, "tables": tables, "w_first": w_first, "b_first": b_first, "w_out": w_out}


def pool_table(inputs):
    table_rows, bag_ids, live_count = inputs
    gathered = jnp.take(table_rows, bag_ids, axis=0).astype(jnp.float32)
    slot_live = (jnp.arange(POOL) < live_count).astype(jnp.float32)
    row_block = bag_ids // ROWS_DEV
    owners = (row_block[:, :, None] == jnp.arange(RSPLIT)[None, None, :]).astype(jnp.float32)
    owners = owners * slot_live[None, :, None]
    partial_value = jnp.einsum('bpr,bpe->rbe', owners, gathered).astype(jnp.bfloat16)
    return jnp.sum(partial_value.astype(jnp.float32), axis=0).astype(jnp.bfloat16)


def reference(indices, pool_len, tables, w_first, b_first, w_out):
    table_view = tables.reshape(TABLES, ROWS, E)
    pooled = lax.map(pool_table, (table_view, jnp.transpose(indices, (1, 0, 2)), pool_len))
    flat_feat = jnp.transpose(pooled, (1, 0, 2)).reshape(BATCH, FEAT)
    pre_act = jnp.dot(flat_feat, w_first, preferred_element_type=jnp.float32) + b_first.astype(jnp.float32)
    hidden = jnp.maximum(pre_act, 0.0)
    return jnp.sum(hidden * w_out.astype(jnp.float32)[None, :], axis=1)
```

```python
import functools

import jax
import jax.numpy as jnp
from jax import lax
from jax.experimental import pallas as pl
from jax.experimental.pallas import tpu as pltpu
from jax.sharding import PartitionSpec as P

VMEM_LIMIT = 60 * 1024 * 1024


def bag_kernel(table_chunks, bags_per_step, pool_size, table_ref, ids_ref, out_ref, staged, wide, sums, sems):
    rows, _ = table_ref.shape
    chunk = rows // table_chunks

    def fetch(c):
        return pltpu.make_async_copy(table_ref.at[pl.ds(c * chunk, chunk)], staged.at[c % 2], sems.at[c % 2])

    fetch(0).start()
    wide[pl.ds(rows, 8), :] = jnp.zeros((8, wide.shape[1]), jnp.float32)
    for c in range(table_chunks):
        if c + 1 < table_chunks:
            fetch(c + 1).start()
        fetch(c).wait()
        step = 256

        def widen(k, carry):
            at = pl.multiple_of(k * step, step)
            wide[pl.ds(c * chunk + at, step), :] = staged[c % 2, pl.ds(at, step), :].astype(jnp.float32)
            return carry

        lax.fori_loop(0, chunk // step, widen, 0)

    def bags(r, carry):
        for b in range(bags_per_step):
            total = None
            for p in range(pool_size):
                row = wide[pl.ds(ids_ref[r, b * pool_size + p], 1), :]
                total = row if total is None else total + row
            sums[pl.ds(r * bags_per_step + b, 1), :] = total
        return carry

    lax.fori_loop(0, ids_ref.shape[0], bags, 0)
    out_ref[...] = sums[...].astype(jnp.bfloat16)


def pool_bags(table, ids, pool_size):
    rows, emb = table.shape
    bags_per_step = ids.shape[1] // pool_size
    n_bags = ids.shape[0] * bags_per_step
    chunks = 8
    return pl.pallas_call(
        functools.partial(bag_kernel, chunks, bags_per_step, pool_size),
        out_shape=jax.ShapeDtypeStruct((n_bags, emb), jnp.bfloat16),
        in_specs=[pl.BlockSpec(memory_space=pl.ANY), pl.BlockSpec(memory_space=pltpu.SMEM)],
        out_specs=pl.BlockSpec(memory_space=pltpu.VMEM),
        scratch_shapes=[
            pltpu.VMEM((2, rows // chunks, emb), jnp.bfloat16),
            pltpu.VMEM((rows + 8, emb), jnp.float32),
            pltpu.VMEM((n_bags, emb), jnp.float32),
            pltpu.SemaphoreType.DMA((2,)),
        ],
        compiler_params=pltpu.CompilerParams(vmem_limit_bytes=VMEM_LIMIT),
        cost_estimate=pl.CostEstimate(flops=n_bags * pool_size * emb * 600, bytes_accessed=rows * emb * 2, transcendentals=0),
        name="pool_bags",
    )(table, ids)


def step_kernel(
    secs, devs, pool_size,
    ids_ref, len_ref, table_ref, w_ref, b_ref, wo_ref, out_ref,
    ids_raw, ids_in, ids_safe, ids_smem, bias, project, staged, wide, sums, pooled, feats, weights, pre, outgoing, first_in, relay, second_in, mine, theirs,
    isend, irecv, icopy, scopy, vsem, tsem, fsend, ysend, dsend, frecv, wsend, wrecv, wlocal, asend, arecv, bsend, brecv, lsend, lrecv,
):
    rows, emb = table_ref.shape
    count = secs * devs
    per_dev, hid = w_ref.shape
    quarter = hid // 2
    chunks, samples, depth = feats.shape
    tiles = wsend.shape[1]
    tile = quarter // tiles
    bags_src = ids_ref.shape[2]
    sec, dev = lax.axis_index("section"), lax.axis_index("dev")
    me = sec * devs + dev
    z, y, x = dev // 4, lax.rem(dev // 2, 2), lax.rem(dev, 2)
    zh, zl = z // 2, lax.rem(z, 2)

    def device(position):
        return {"section": position // devs, "dev": lax.rem(position, devs)}

    def place(s, zz, yy, xx):
        return {"section": s, "dev": zz * 4 + yy * 2 + xx}

    table_chunks = 8
    piece = rows // table_chunks

    def fetch(c):
        return pltpu.make_async_copy(table_ref.at[pl.ds(c * piece, piece)], staged.at[c % 2], tsem.at[c % 2])

    barrier = pltpu.get_barrier_semaphore()
    for k in range(1, count):
        pl.semaphore_signal(barrier, inc=1, device_id=device(lax.rem(me + k, count)))

    raw_ids = pltpu.make_async_copy(ids_ref, ids_raw, icopy)
    raw_ids.start()
    small = [
        pltpu.make_async_copy(b_ref, bias, vsem.at[0]),
        pltpu.make_async_copy(wo_ref, project, vsem.at[1]),
    ]
    for copy in small:
        copy.start()
    fetch(0).start()
    own_slot = zl * 2 + y
    own_cols = pl.ds(pl.multiple_of(y * quarter, quarter), quarter)
    own_weights = pltpu.make_async_copy(w_ref.at[:, own_cols], weights.at[own_slot], wlocal)
    own_weights.start()
    raw_ids.wait()
    slot_row = lax.broadcasted_iota(jnp.int32, ids_ref.shape[1:], 0)
    for t in range(count):
        ids_safe[t] = jnp.where(slot_row < len_ref[t], ids_raw[t], rows)
    wide[pl.ds(rows, 8), :] = jnp.zeros((8, emb), jnp.float32)
    step = 256
    for c in range(table_chunks):
        if c + 1 < table_chunks:
            fetch(c + 1).start()
        fetch(c).wait()

        def widen(k, carry):
            at = pl.multiple_of(k * step, step)
            wide[pl.ds(c * piece + at, step), :] = staged[c % 2, pl.ds(at, step), :].astype(jnp.float32)
            return carry

        lax.fori_loop(0, piece // step, widen, 0)

    pl.semaphore_wait(barrier, count - 1)

    my_pair = me // 2
    my_zh, my_u, my_x, my_h = my_pair // 8, lax.rem(my_pair // 2, 4), lax.rem(my_pair, 2), lax.rem(me, 2)
    my_place = ids_in.at[my_zh, my_u, my_x, pl.ds(pl.multiple_of(my_h * pool_size, pool_size), pool_size)]

    def turn(position):
        near_x = lax.rem(lax.rem(lax.rem(position, devs) // 2, 2) + my_x + 1, 2)
        return near_x + 2 * lax.rem(position // devs + my_zh + 1, 2)

    own_ids = pltpu.make_async_copy(ids_safe.at[me], my_place, irecv.at[turn(me)])
    own_ids.start()
    for k in range(1, count):
        other = lax.rem(me + k, count)
        pltpu.make_async_remote_copy(
            src_ref=ids_safe.at[other], dst_ref=my_place, send_sem=isend, recv_sem=irecv.at[turn(other)],
            device_id=device(other),
        ).start()

    started = []
    shipped = {}

    def ship(r, n):
        cols = pl.ds(n * tile, tile)
        if r == 1:
            source = w_ref.at[:, pl.ds(pl.multiple_of((1 - y) * quarter + n * tile, tile), tile)]
        elif r == 2:
            source = w_ref.at[:, pl.ds(pl.multiple_of(y * quarter + n * tile, tile), tile)]
        else:
            shipped[1, n].wait_recv()
            source = weights.at[zl * 2 + 1 - y, :, cols]
        slot = zl * 2 + 1 - y if r == 3 else own_slot
        copy = pltpu.make_async_remote_copy(
            src_ref=source, dst_ref=weights.at[slot, :, cols],
            send_sem=wsend.at[r - 1, n], recv_sem=wrecv.at[r - 1, n],
            device_id=place(sec, z, 1 - y, x) if r == 1 else place(sec, zh * 2 + 1 - zl, y, x),
        )
        copy.start()
        started.append(copy)
        shipped[r, n] = copy

    for n in range(tiles):
        ship(1, n)
        ship(2, n)

    def part_of(j, c):
        return feats.at[j, :, pl.ds(pl.multiple_of(c * emb, emb), emb)]

    def landed(j, c):
        part = part_of(j, c)
        pltpu.make_async_copy(part, part, frecv.at[j, c]).wait()
        return part

    def across(j, c, lane):
        part = part_of(j, c)
        copy = pltpu.make_async_remote_copy(
            src_ref=part, dst_ref=part, send_sem=dsend.at[j, lane], recv_sem=frecv.at[j, c],
            device_id=place(1 - sec, z, y, x),
        )
        copy.start()
        started.append(copy)

    def forward(j):
        for i in range(2):
            c = (sec + 2 * i) * 2 + lax.rem(y + j, 2)
            part = landed(j, c)
            copy = pltpu.make_async_remote_copy(
                src_ref=part, dst_ref=part, send_sem=ysend.at[j, i], recv_sem=frecv.at[j, c],
                device_id=place(sec, z, 1 - y, x),
            )
            copy.start()
            started.append(copy)
            across(j, c, i)

    def share(j):
        for i in range(2):
            c = (sec + 2 * i) * 2 + lax.rem(y + j + 1, 2)
            landed(j, c)
            across(j, c, 2 + i)

    def complete(j):
        for i in range(2):
            for b in range(2):
                landed(j, (1 - sec + 2 * i) * 2 + b)

    column = z * 2 + x
    kept = []
    def stage_ids(j):
        to_x = 1 - y if j % 2 == 0 else y
        to_zh = 1 - sec if j < 2 else sec
        ids_part = ids_in.at[to_zh, :, to_x]
        pltpu.make_async_copy(ids_part, ids_part, irecv.at[j]).wait()
        lines = [
            pltpu.make_async_copy(
                ids_part.at[u], ids_smem.at[j % 2, pl.ds(2 * pool_size * u, 2 * pool_size)], scopy.at[j % 2, u]
            )
            for u in range(4)
        ]
        for copy in lines:
            copy.start()
        return lines

    staged_ids = {0: stage_ids(0)}

    def pool(j, half):
        def bags(u, lines):
            for b in range(bags_src):
                total = None
                for p in range(pool_size):
                    row = wide[pl.ds(ids_smem[j % 2, lines[p], b], 1), :]
                    total = row if total is None else total + row
                sums[u, pl.ds(b, 1), :] = total
            return tuple(line + pool_size for line in lines)

        start = 4 * half
        lax.fori_loop(start, start + 4, bags, tuple(jnp.int32(start * pool_size + p) for p in range(pool_size)))
        pooled[j, half] = sums[start:start + 4].astype(jnp.bfloat16).reshape(samples, emb)
        dst = part_of(j, column)
        copy = pltpu.make_async_remote_copy(
            src_ref=pooled.at[j, half], dst_ref=dst, send_sem=fsend.at[j, half], recv_sem=frecv.at[j, column],
            device_id=place(lax.rem(z, 2), 2 * sec + half, lax.rem(x + j, 2), y),
        )
        local = pltpu.make_async_copy(pooled.at[j, half], dst, frecv.at[j, column])
        keeps = jnp.logical_and(
            jnp.logical_and(lax.rem(z, 2) == sec, 2 * sec + half == z),
            jnp.logical_and(x == y, lax.rem(x + j, 2) == y),
        )

        @pl.when(keeps)
        def _():
            local.start()

        @pl.when(jnp.logical_not(keeps))
        def _():
            copy.start()

        kept.append((keeps, copy))

    for j in range(chunks):
        for copy in staged_ids[j]:
            copy.wait()
        if j + 1 < chunks:
            staged_ids[j + 1] = stage_ids(j + 1)
        pool(j, 0)
        if j < 2:
            ship(3, 2 * j)
            ship(3, 2 * j + 1)
        pool(j, 1)
        if j >= 1:
            forward(j - 1)
        if j >= 2:
            share(j - 2)

    own_weights.wait()
    first, second = {}, {}

    def multiply(j, n):
        cols = pl.ds(n * tile, tile)
        return jnp.dot(
            feats[j], weights[:, :, cols].reshape(depth, tile), preferred_element_type=jnp.float32
        )

    def give(b, n):
        cols = pl.ds(n * tile, tile)
        outgoing[b, :, cols] = multiply(2 * b, n).astype(jnp.bfloat16)
        copy = pltpu.make_async_remote_copy(
            src_ref=outgoing.at[b, :, cols], dst_ref=first_in.at[b, :, cols],
            send_sem=asend.at[b, n], recv_sem=arecv.at[b, n], device_id=place(sec, z, y, 1 - x),
        )
        copy.start()
        started.append(copy)
        first[b, n] = copy

    def hand_on(n):
        cols = pl.ds(n * tile, tile)
        first[0, n].wait_recv()
        relay[:, cols] = (pre[0, :, cols] + first_in[0, :, cols].astype(jnp.float32)).astype(jnp.bfloat16)
        copy = pltpu.make_async_remote_copy(
            src_ref=relay.at[:, cols], dst_ref=second_in.at[:, cols],
            send_sem=bsend.at[n], recv_sem=brecv.at[n],
            device_id=place(sec, lax.rem(z + 2, 4), y, x),
        )
        copy.start()
        started.append(copy)
        second[n] = copy

    complete(0)
    for n in range(tiles):
        for r in (2, 3):
            shipped[r, n].wait_recv()
        give(0, n)
    forward(3)
    share(2)
    complete(1)
    for n in range(tiles):
        pre[0, :, pl.ds(n * tile, tile)] = multiply(1, n)
    share(3)
    complete(2)
    for n in range(tiles):
        give(1, n)
        hand_on(n)
    complete(3)
    for n in range(tiles):
        pre[1, :, pl.ds(n * tile, tile)] = multiply(3, n)

    for copy in small:
        copy.wait()
    acc = jnp.zeros((samples, 128), jnp.float32)
    for n in range(tiles):
        cols = pl.ds(n * tile, tile)
        other = pl.ds(quarter + n * tile, tile)
        first[1, n].wait_recv()
        total = pre[1, :, cols] + first_in[1, :, cols].astype(jnp.float32)
        second[n].wait_recv()
        total = total + second_in[:, cols].astype(jnp.float32)
        shift = jnp.where(y == 0, bias[cols].astype(jnp.float32), bias[other].astype(jnp.float32))
        scale = jnp.where(y == 0, project[cols].astype(jnp.float32), project[other].astype(jnp.float32))
        hidden = jnp.maximum(total + shift[None, :], 0.0)
        weighed = hidden * scale[None, :]
        for q in range(tile // 128):
            acc = acc + weighed[:, q * 128:(q + 1) * 128]
    logits = jnp.sum(acc.T, axis=0, keepdims=True)
    half = samples // 2
    for b in range(2):
        mine[b] = logits[:, b * half:(b + 1) * half]
    swaps = []
    for r in (1, 2, 3):
        to_y = 1 - y if r & 1 else y
        to_sec = 1 - sec if r & 2 else sec
        swap = pltpu.make_async_remote_copy(
            src_ref=mine.at[to_y], dst_ref=theirs.at[r - 1], send_sem=lsend.at[r - 1], recv_sem=lrecv.at[r - 1],
            device_id=place(to_sec, z, to_y, x),
        )
        swap.start()
        swaps.append(swap)
    for swap in swaps:
        swap.wait_recv()
    out_ref[...] = mine[y] + theirs[0] + theirs[1] + theirs[2]
    for copy in started + swaps:
        copy.wait_send()
    for keeps, copy in kept:

        @pl.when(jnp.logical_not(keeps))
        def _():
            copy.wait_send()

    sent = ids_safe.at[pl.ds(0, count - 1)]
    pltpu.make_async_copy(sent, sent, isend).wait()


def whole_step(secs, devs, pool_size, ids, pool_len, table, w_first, bias, w_out):
    rows, emb = table.shape
    per_dev, hid = w_first.shape
    quarter = hid // 2
    bags_src = ids.shape[2]
    samples = 4 * bags_src
    depth = 4 * per_dev
    tiles = 4
    columns = depth // emb
    vm = pl.BlockSpec(memory_space=pltpu.VMEM)
    anywhere = pl.BlockSpec(memory_space=pl.ANY)
    dma = pltpu.SemaphoreType.DMA
    return pl.pallas_call(
        functools.partial(step_kernel, secs, devs, pool_size),
        out_shape=jax.ShapeDtypeStruct((1, samples // 2), jnp.float32),
        in_specs=[anywhere, pl.BlockSpec(memory_space=pltpu.SMEM), anywhere, anywhere, anywhere, anywhere],
        out_specs=vm,
        scratch_shapes=[
            pltpu.VMEM(ids.shape, jnp.int32),
            pltpu.VMEM((2, 4, 2, 2 * pool_size, bags_src), jnp.int32),
            pltpu.VMEM(ids.shape, jnp.int32),
            pltpu.SMEM((2, 8 * pool_size, bags_src), jnp.int32),
            pltpu.VMEM((hid,), jnp.bfloat16),
            pltpu.VMEM((hid,), jnp.bfloat16),
            pltpu.VMEM((2, rows // 8, emb), jnp.bfloat16),
            pltpu.VMEM((rows + 8, emb), jnp.float32),
            pltpu.VMEM((8, bags_src, emb), jnp.float32),
            pltpu.VMEM((4, 2, samples, emb), jnp.bfloat16),
            pltpu.VMEM((4, samples, depth), jnp.bfloat16),
            pltpu.VMEM((4, per_dev, quarter), jnp.bfloat16),
            pltpu.VMEM((2, samples, quarter), jnp.float32),
            pltpu.VMEM((2, samples, quarter), jnp.bfloat16),
            pltpu.VMEM((2, samples, quarter), jnp.bfloat16),
            pltpu.VMEM((samples, quarter), jnp.bfloat16),
            pltpu.VMEM((samples, quarter), jnp.bfloat16),
            pltpu.VMEM((2, 1, samples // 2), jnp.float32),
            pltpu.VMEM((3, 1, samples // 2), jnp.float32),
            dma, dma((4,)), dma, dma((2, 4)), dma((2,)), dma((2,)),
            dma((4, 2)), dma((4, 2)), dma((4, 4)), dma((4, columns)),
            dma((3, tiles)), dma((3, tiles)), dma,
            dma((2, tiles)), dma((2, tiles)), dma((tiles,)), dma((tiles,)),
            dma((3,)), dma((3,)),
        ],
        compiler_params=pltpu.CompilerParams(collective_id=0, has_side_effects=True, vmem_limit_bytes=VMEM_LIMIT),
        name="whole_step",
    )(ids, pool_len, table, w_first, bias, w_out)


def body(indices, pool_len, tables, w_first, b_first, w_out):
    sec_count = lax.axis_size("section")
    dev_count = lax.axis_size("dev")
    devices = sec_count * dev_count
    dev_rows, n_tables, pool_size = indices.shape
    rows_dev, emb_width = tables.shape
    row_split = devices // n_tables
    position = lax.axis_index("section") * dev_count + lax.axis_index("dev")
    table_id = position // row_split
    first_row = position % row_split * rows_dev
    square = row_split == 1 and sec_count == 2 and dev_count == 16
    if square and w_first.shape[0] == 2 * emb_width and w_first.shape[1] % 2048 == 0 and dev_rows % 64 == 0:
        ids = jnp.transpose(indices, (1, 2, 0))
        logits = whole_step(
            sec_count, dev_count, pool_size, ids, pool_len, tables, w_first, b_first, w_out
        )
        return logits.reshape(logits.shape[1])
    outgoing = jnp.transpose(indices, (1, 0, 2)).reshape(n_tables, dev_rows * pool_size)
    outgoing = jnp.repeat(outgoing, row_split, axis=0)
    arrived = lax.all_to_all(outgoing, ("section", "dev"), split_axis=0, concat_axis=0, tiled=True)
    all_rows = devices * dev_rows
    wanted = arrived.reshape(all_rows * pool_size // 128, 128) - first_row
    live_slots = jnp.sum(jnp.where(jnp.arange(n_tables) == table_id, pool_len, 0))
    slot = jnp.arange(128) % pool_size
    usable = (wanted >= 0) & (wanted < rows_dev) & (slot < live_slots)[None, :]
    safe_rows = jnp.where(usable, wanted, rows_dev)
    partial_value = pool_bags(tables, safe_rows, pool_size)
    ordered = jnp.transpose(
        partial_value.reshape(dev_count, sec_count, dev_rows, emb_width), (1, 0, 2, 3)
    )
    received = lax.all_to_all(
        ordered.reshape(devices, dev_rows, emb_width),
        ("section", "dev"),
        split_axis=0,
        concat_axis=0,
        tiled=True,
    )
    summed = jnp.sum(
        received.reshape(n_tables, row_split, dev_rows, emb_width).astype(jnp.float32), axis=1
    )
    features = jnp.transpose(summed.astype(jnp.bfloat16), (1, 0, 2)).reshape(
        dev_rows, n_tables * emb_width
    )
    samples = lax.all_gather(features, "section", axis=0, tiled=True)
    whole_weights = lax.all_gather(w_first, "dev", axis=0, tiled=True)
    pre_act = jnp.dot(samples, whole_weights, preferred_element_type=jnp.float32)
    hidden = jnp.maximum(pre_act + b_first.astype(jnp.float32)[None, :], 0.0)
    logit_part = jnp.sum(hidden * w_out.astype(jnp.float32)[None, :], axis=1)
    return lax.psum(logit_part, "section")


def solution(mesh):
    placed = (
        P(("section", "dev"), None, None),
        P(),
        P(("section", "dev"), None),
        P("dev", "section"),
        P("section"),
        P("section"),
    )
    return jax.shard_map(body, mesh=mesh, in_specs=placed, out_specs=P("dev"), check_vma=False)
```

```python
import functools

import jax
import jax.numpy as jnp
from jax import lax
from jax.experimental import pallas as pl
from jax.experimental.pallas import tpu as pltpu
from jax.sharding import PartitionSpec as P

VMEM_LIMIT = 60 * 1024 * 1024
RELAYED = (((3, 0),), ((3, 1), (2, 2)), ((3, 2),), ((2, 3), (3, 3)))


def bag_kernel(table_chunks, bags_per_step, pool_size, table_ref, ids_ref, out_ref, staged, wide, sums, sems):
    rows, _ = table_ref.shape
    chunk = rows // table_chunks

    def fetch(c):
        return pltpu.make_async_copy(table_ref.at[pl.ds(c * chunk, chunk)], staged.at[c % 2], sems.at[c % 2])

    fetch(0).start()
    wide[pl.ds(rows, 8), :] = jnp.zeros((8, wide.shape[1]), jnp.float32)
    for c in range(table_chunks):
        if c + 1 < table_chunks:
            fetch(c + 1).start()
        fetch(c).wait()
        step = 256

        def widen(k, carry):
            at = pl.multiple_of(k * step, step)
            wide[pl.ds(c * chunk + at, step), :] = staged[c % 2, pl.ds(at, step), :].astype(jnp.float32)
            return carry

        lax.fori_loop(0, chunk // step, widen, 0)

    def bags(r, carry):
        for b in range(bags_per_step):
            total = None
            for p in range(pool_size):
                row = wide[pl.ds(ids_ref[r, b * pool_size + p], 1), :]
                total = row if total is None else total + row
            sums[pl.ds(r * bags_per_step + b, 1), :] = total
        return carry

    lax.fori_loop(0, ids_ref.shape[0], bags, 0)
    out_ref[...] = sums[...].astype(jnp.bfloat16)


def pool_bags(table, ids, pool_size):
    rows, emb = table.shape
    bags_per_step = ids.shape[1] // pool_size
    n_bags = ids.shape[0] * bags_per_step
    chunks = 8
    return pl.pallas_call(
        functools.partial(bag_kernel, chunks, bags_per_step, pool_size),
        out_shape=jax.ShapeDtypeStruct((n_bags, emb), jnp.bfloat16),
        in_specs=[pl.BlockSpec(memory_space=pl.ANY), pl.BlockSpec(memory_space=pltpu.SMEM)],
        out_specs=pl.BlockSpec(memory_space=pltpu.VMEM),
        scratch_shapes=[
            pltpu.VMEM((2, rows // chunks, emb), jnp.bfloat16),
            pltpu.VMEM((rows + 8, emb), jnp.float32),
            pltpu.VMEM((n_bags, emb), jnp.float32),
            pltpu.SemaphoreType.DMA((2,)),
        ],
        compiler_params=pltpu.CompilerParams(vmem_limit_bytes=VMEM_LIMIT),
        cost_estimate=pl.CostEstimate(flops=n_bags * pool_size * emb * 600, bytes_accessed=rows * emb * 2, transcendentals=0),
        name="pool_bags",
    )(table, ids)


def step_kernel(
    secs, devs, pool_size,
    ids_ref, len_ref, table_ref, w_ref, b_ref, wo_ref, out_ref,
    ids_raw, ids_in, ids_safe, ids_smem, bias, project, staged, wide, sums, pooled, feats, weights, pre, outgoing, first_in, relay, second_in, mine, theirs,
    isend, irecv, icopy, scopy, vsem, tsem, fsend, ysend, dsend, frecv, wsend, wrecv, wlocal, asend, arecv, bsend, brecv, lsend, lrecv,
):
    rows, emb = table_ref.shape
    count = secs * devs
    per_dev, hid = w_ref.shape
    quarter = hid // 2
    chunks, samples, depth = feats.shape
    tiles = wsend.shape[1]
    tile = quarter // tiles
    width = quarter // asend.shape[1]
    pieces = tile // width
    bags_src = ids_ref.shape[2]
    sec, dev = lax.axis_index("section"), lax.axis_index("dev")
    me = sec * devs + dev
    z, y, x = dev // 4, lax.rem(dev // 2, 2), lax.rem(dev, 2)
    zh, zl = z // 2, lax.rem(z, 2)

    def device(position):
        return {"section": position // devs, "dev": lax.rem(position, devs)}

    def place(s, zz, yy, xx):
        return {"section": s, "dev": zz * 4 + yy * 2 + xx}

    table_chunks = 8
    piece = rows // table_chunks

    def fetch(c):
        return pltpu.make_async_copy(table_ref.at[pl.ds(c * piece, piece)], staged.at[c % 2], tsem.at[c % 2])

    barrier = pltpu.get_barrier_semaphore()
    for k in range(1, count):
        pl.semaphore_signal(barrier, inc=1, device_id=device(lax.rem(me + k, count)))

    raw_ids = pltpu.make_async_copy(ids_ref, ids_raw, icopy)
    raw_ids.start()
    small = [
        pltpu.make_async_copy(b_ref, bias, vsem.at[0]),
        pltpu.make_async_copy(wo_ref, project, vsem.at[1]),
    ]
    for copy in small:
        copy.start()
    fetch(0).start()
    own_slot = zl * 2 + y
    own_cols = pl.ds(pl.multiple_of(y * quarter, quarter), quarter)
    own_weights = pltpu.make_async_copy(w_ref.at[:, own_cols], weights.at[own_slot], wlocal)
    own_weights.start()
    raw_ids.wait()
    slot_row = lax.broadcasted_iota(jnp.int32, ids_ref.shape[1:], 0)
    for t in range(count):
        ids_safe[t] = jnp.where(slot_row < len_ref[t], ids_raw[t], rows)
    wide[pl.ds(rows, 8), :] = jnp.zeros((8, emb), jnp.float32)
    step = 256
    for c in range(table_chunks):
        if c + 1 < table_chunks:
            fetch(c + 1).start()
        fetch(c).wait()

        def widen(k, carry):
            at = pl.multiple_of(k * step, step)
            wide[pl.ds(c * piece + at, step), :] = staged[c % 2, pl.ds(at, step), :].astype(jnp.float32)
            return carry

        lax.fori_loop(0, piece // step, widen, 0)

    pl.semaphore_wait(barrier, count - 1)

    my_pair = me // 2
    my_zh, my_u, my_x, my_h = my_pair // 8, lax.rem(my_pair // 2, 4), lax.rem(my_pair, 2), lax.rem(me, 2)
    my_place = ids_in.at[my_zh, my_u, my_x, pl.ds(pl.multiple_of(my_h * pool_size, pool_size), pool_size)]

    for j in range(4):
        for i in range(8):
            to_sec = 1 - my_zh if j < 2 else my_zh
            to_y = 1 - my_x if j % 2 == 0 else my_x
            to_z = lax.rem(z + 2 + i // 2, 4)
            other = to_sec * devs + to_z * 4 + to_y * 2 + i % 2
            remote = pltpu.make_async_remote_copy(
                src_ref=ids_safe.at[other], dst_ref=my_place, send_sem=isend, recv_sem=irecv.at[j],
                device_id=device(other),
            )
            own_ids = pltpu.make_async_copy(ids_safe.at[me], my_place, irecv.at[j])

            @pl.when(other == me)
            def _():
                own_ids.start()

            @pl.when(other != me)
            def _():
                remote.start()

    started = []
    shipped = {}

    def ship(r, n):
        cols = pl.ds(n * tile, tile)
        if r == 1:
            source = w_ref.at[:, pl.ds(pl.multiple_of((1 - y) * quarter + n * tile, tile), tile)]
        elif r == 2:
            source = w_ref.at[:, pl.ds(pl.multiple_of(y * quarter + n * tile, tile), tile)]
        else:
            shipped[1, n].wait_recv()
            source = weights.at[zl * 2 + 1 - y, :, cols]
        slot = zl * 2 + 1 - y if r == 3 else own_slot
        copy = pltpu.make_async_remote_copy(
            src_ref=source, dst_ref=weights.at[slot, :, cols],
            send_sem=wsend.at[r - 1, n], recv_sem=wrecv.at[r - 1, n],
            device_id=place(sec, z, 1 - y, x) if r == 1 else place(sec, zh * 2 + 1 - zl, y, x),
        )
        copy.start()
        started.append(copy)
        shipped[r, n] = copy

    for n in range(tiles):
        ship(1, n)
        if n < 2:
            ship(2, n)

    def part_of(j, c):
        return feats.at[j, :, pl.ds(pl.multiple_of(c * emb, emb), emb)]

    def landed(j, c):
        part = part_of(j, c)
        pltpu.make_async_copy(part, part, frecv.at[j, c]).wait()
        return part

    def across(j, c, lane):
        part = part_of(j, c)
        copy = pltpu.make_async_remote_copy(
            src_ref=part, dst_ref=part, send_sem=dsend.at[j, lane], recv_sem=frecv.at[j, c],
            device_id=place(1 - sec, z, y, x),
        )
        copy.start()
        started.append(copy)

    def forward(j):
        for i in range(2):
            c = (sec + 2 * i) * 2 + lax.rem(y + j, 2)
            part = landed(j, c)
            copy = pltpu.make_async_remote_copy(
                src_ref=part, dst_ref=part, send_sem=ysend.at[j, i], recv_sem=frecv.at[j, c],
                device_id=place(sec, z, 1 - y, x),
            )
            copy.start()
            started.append(copy)
            across(j, c, i)

    def share(j):
        for i in range(2):
            c = (sec + 2 * i) * 2 + lax.rem(y + j + 1, 2)
            landed(j, c)
            across(j, c, 2 + i)

    def complete(j):
        for i in range(2):
            for b in range(2):
                landed(j, (1 - sec + 2 * i) * 2 + b)

    column = z * 2 + x
    kept = []
    def stage_ids(j):
        to_x = 1 - y if j % 2 == 0 else y
        to_zh = 1 - sec if j < 2 else sec
        ids_part = ids_in.at[to_zh, :, to_x]
        pltpu.make_async_copy(ids_part, ids_part, irecv.at[j]).wait()
        lines = [
            pltpu.make_async_copy(
                ids_part.at[u], ids_smem.at[j % 2, pl.ds(2 * pool_size * u, 2 * pool_size)], scopy.at[j % 2, u]
            )
            for u in range(4)
        ]
        for copy in lines:
            copy.start()
        return lines

    staged_ids = {0: stage_ids(0)}

    def pool(j, half):
        def bags(u, lines):
            for b in range(bags_src):
                total = None
                for p in range(pool_size):
                    row = wide[pl.ds(ids_smem[j % 2, lines[p], b], 1), :]
                    total = row if total is None else total + row
                sums[u, pl.ds(b, 1), :] = total
            return tuple(line + pool_size for line in lines)

        start = 4 * half
        lax.fori_loop(start, start + 4, bags, tuple(jnp.int32(start * pool_size + p) for p in range(pool_size)))
        pooled[j, half] = sums[start:start + 4].astype(jnp.bfloat16).reshape(samples, emb)
        dst = part_of(j, column)
        copy = pltpu.make_async_remote_copy(
            src_ref=pooled.at[j, half], dst_ref=dst, send_sem=fsend.at[j, half], recv_sem=frecv.at[j, column],
            device_id=place(lax.rem(z, 2), 2 * sec + half, lax.rem(x + j, 2), y),
        )
        local = pltpu.make_async_copy(pooled.at[j, half], dst, frecv.at[j, column])
        keeps = jnp.logical_and(
            jnp.logical_and(lax.rem(z, 2) == sec, 2 * sec + half == z),
            jnp.logical_and(x == y, lax.rem(x + j, 2) == y),
        )

        @pl.when(keeps)
        def _():
            local.start()

        @pl.when(jnp.logical_not(keeps))
        def _():
            copy.start()

        kept.append((keeps, copy))

    for j in range(chunks):
        for copy in staged_ids[j]:
            copy.wait()
        if j + 1 < chunks:
            staged_ids[j + 1] = stage_ids(j + 1)
        pool(j, 0)
        if j == 3:
            forward(1)
        pool(j, 1)
        if j == 2:
            forward(0)
        for r, n in RELAYED[j]:
            ship(r, n)

    own_weights.wait()
    first, second = {}, {}

    def multiply(j, n):
        cols = pl.ds(n * tile, tile)
        return jnp.dot(
            feats[j], weights[:, :, cols].reshape(depth, tile), preferred_element_type=jnp.float32
        )

    def give(b, n):
        cols = pl.ds(n * tile, tile)
        outgoing[b, :, cols] = multiply(2 * b, n).astype(jnp.bfloat16)
        for m in range(n * pieces, (n + 1) * pieces):
            cols = pl.ds(m * width, width)
            copy = pltpu.make_async_remote_copy(
                src_ref=outgoing.at[b, :, cols], dst_ref=first_in.at[b, :, cols],
                send_sem=asend.at[b, m], recv_sem=arecv.at[b, m], device_id=place(sec, z, y, 1 - x),
            )
            copy.start()
            started.append(copy)
            first[b, m] = copy

    def hand_on(n):
        for m in range(n * pieces, (n + 1) * pieces):
            cols = pl.ds(m * width, width)
            first[0, m].wait_recv()
            relay[:, cols] = (pre[0, :, cols] + first_in[0, :, cols].astype(jnp.float32)).astype(jnp.bfloat16)
            copy = pltpu.make_async_remote_copy(
                src_ref=relay.at[:, cols], dst_ref=second_in.at[:, cols],
                send_sem=bsend.at[m], recv_sem=brecv.at[m],
                device_id=place(sec, lax.rem(z + 2, 4), y, x),
            )
            copy.start()
            started.append(copy)
            second[m] = copy

    def keep(b, n):
        pre[b, :, pl.ds(n * tile, tile)] = multiply(2 * b + 1, n)

    def lead(n):
        for r in (2, 3):
            shipped[r, n].wait_recv()
        give(0, n)

    share(0)
    complete(0)
    lead(0)
    lead(1)
    share(1)
    forward(2)
    complete(1)
    keep(0, 0)
    hand_on(0)
    keep(0, 1)
    lead(2)
    hand_on(1)
    forward(3)
    share(2)
    lead(3)
    keep(0, 2)
    hand_on(2)
    keep(0, 3)
    complete(2)
    give(1, 0)
    hand_on(3)
    give(1, 1)
    give(1, 2)
    share(3)
    give(1, 3)
    complete(3)
    for n in range(tiles):
        keep(1, n)

    for copy in small:
        copy.wait()
    acc = jnp.zeros((samples, 128), jnp.float32)
    for m in range(quarter // width):
        cols, other = pl.ds(m * width, width), pl.ds(quarter + m * width, width)
        first[1, m].wait_recv()
        total = pre[1, :, cols] + first_in[1, :, cols].astype(jnp.float32)
        second[m].wait_recv()
        total = total + second_in[:, cols].astype(jnp.float32)
        shift = jnp.where(y == 0, bias[cols].astype(jnp.float32), bias[other].astype(jnp.float32))
        scale = jnp.where(y == 0, project[cols].astype(jnp.float32), project[other].astype(jnp.float32))
        hidden = jnp.maximum(total + shift[None, :], 0.0)
        weighed = hidden * scale[None, :]
        for q in range(width // 128):
            acc = acc + weighed[:, q * 128:(q + 1) * 128]
    logits = jnp.sum(acc.T, axis=0, keepdims=True)
    half = samples // 2
    for b in range(2):
        mine[b] = logits[:, b * half:(b + 1) * half]
    swaps = []
    for r in (1, 2, 3):
        to_y = 1 - y if r & 1 else y
        to_sec = 1 - sec if r & 2 else sec
        swap = pltpu.make_async_remote_copy(
            src_ref=mine.at[to_y], dst_ref=theirs.at[r - 1], send_sem=lsend.at[r - 1], recv_sem=lrecv.at[r - 1],
            device_id=place(to_sec, z, to_y, x),
        )
        swap.start()
        swaps.append(swap)
    for swap in swaps:
        swap.wait_recv()
    out_ref[...] = mine[y] + theirs[0] + theirs[1] + theirs[2]
    for copy in started + swaps:
        copy.wait_send()
    for keeps, copy in kept:

        @pl.when(jnp.logical_not(keeps))
        def _():
            copy.wait_send()

    sent = ids_safe.at[pl.ds(0, count - 1)]
    pltpu.make_async_copy(sent, sent, isend).wait()


def whole_step(secs, devs, pool_size, ids, pool_len, table, w_first, bias, w_out):
    rows, emb = table.shape
    per_dev, hid = w_first.shape
    quarter = hid // 2
    bags_src = ids.shape[2]
    samples = 4 * bags_src
    depth = 4 * per_dev
    tiles = 4
    parts = 8
    columns = depth // emb
    vm = pl.BlockSpec(memory_space=pltpu.VMEM)
    anywhere = pl.BlockSpec(memory_space=pl.ANY)
    dma = pltpu.SemaphoreType.DMA
    return pl.pallas_call(
        functools.partial(step_kernel, secs, devs, pool_size),
        out_shape=jax.ShapeDtypeStruct((1, samples // 2), jnp.float32),
        in_specs=[anywhere, pl.BlockSpec(memory_space=pltpu.SMEM), anywhere, anywhere, anywhere, anywhere],
        out_specs=vm,
        scratch_shapes=[
            pltpu.VMEM(ids.shape, jnp.int32),
            pltpu.VMEM((2, 4, 2, 2 * pool_size, bags_src), jnp.int32),
            pltpu.VMEM(ids.shape, jnp.int32),
            pltpu.SMEM((2, 8 * pool_size, bags_src), jnp.int32),
            pltpu.VMEM((hid,), jnp.bfloat16),
            pltpu.VMEM((hid,), jnp.bfloat16),
            pltpu.VMEM((2, rows // 8, emb), jnp.bfloat16),
            pltpu.VMEM((rows + 8, emb), jnp.float32),
            pltpu.VMEM((8, bags_src, emb), jnp.float32),
            pltpu.VMEM((4, 2, samples, emb), jnp.bfloat16),
            pltpu.VMEM((4, samples, depth), jnp.bfloat16),
            pltpu.VMEM((4, per_dev, quarter), jnp.bfloat16),
            pltpu.VMEM((2, samples, quarter), jnp.float32),
            pltpu.VMEM((2, samples, quarter), jnp.bfloat16),
            pltpu.VMEM((2, samples, quarter), jnp.bfloat16),
            pltpu.VMEM((samples, quarter), jnp.bfloat16),
            pltpu.VMEM((samples, quarter), jnp.bfloat16),
            pltpu.VMEM((2, 1, samples // 2), jnp.float32),
            pltpu.VMEM((3, 1, samples // 2), jnp.float32),
            dma, dma((4,)), dma, dma((2, 4)), dma((2,)), dma((2,)),
            dma((4, 2)), dma((4, 2)), dma((4, 4)), dma((4, columns)),
            dma((3, tiles)), dma((3, tiles)), dma,
            dma((2, parts)), dma((2, parts)), dma((parts,)), dma((parts,)),
            dma((3,)), dma((3,)),
        ],
        compiler_params=pltpu.CompilerParams(collective_id=0, has_side_effects=True, vmem_limit_bytes=VMEM_LIMIT),
        name="whole_step",
    )(ids, pool_len, table, w_first, bias, w_out)


def body(indices, pool_len, tables, w_first, b_first, w_out):
    sec_count = lax.axis_size("section")
    dev_count = lax.axis_size("dev")
    devices = sec_count * dev_count
    dev_rows, n_tables, pool_size = indices.shape
    rows_dev, emb_width = tables.shape
    row_split = devices // n_tables
    position = lax.axis_index("section") * dev_count + lax.axis_index("dev")
    table_id = position // row_split
    first_row = position % row_split * rows_dev
    square = row_split == 1 and sec_count == 2 and dev_count == 16
    if square and w_first.shape[0] == 2 * emb_width and w_first.shape[1] % 2048 == 0 and dev_rows % 64 == 0:
        ids = jnp.transpose(indices, (1, 2, 0))
        logits = whole_step(
            sec_count, dev_count, pool_size, ids, pool_len, tables, w_first, b_first, w_out
        )
        return logits.reshape(logits.shape[1])
    outgoing = jnp.transpose(indices, (1, 0, 2)).reshape(n_tables, dev_rows * pool_size)
    outgoing = jnp.repeat(outgoing, row_split, axis=0)
    arrived = lax.all_to_all(outgoing, ("section", "dev"), split_axis=0, concat_axis=0, tiled=True)
    all_rows = devices * dev_rows
    wanted = arrived.reshape(all_rows * pool_size // 128, 128) - first_row
    live_slots = jnp.sum(jnp.where(jnp.arange(n_tables) == table_id, pool_len, 0))
    slot = jnp.arange(128) % pool_size
    usable = (wanted >= 0) & (wanted < rows_dev) & (slot < live_slots)[None, :]
    safe_rows = jnp.where(usable, wanted, rows_dev)
    partial_value = pool_bags(tables, safe_rows, pool_size)
    ordered = jnp.transpose(
        partial_value.reshape(dev_count, sec_count, dev_rows, emb_width), (1, 0, 2, 3)
    )
    received = lax.all_to_all(
        ordered.reshape(devices, dev_rows, emb_width),
        ("section", "dev"),
        split_axis=0,
        concat_axis=0,
        tiled=True,
    )
    summed = jnp.sum(
        received.reshape(n_tables, row_split, dev_rows, emb_width).astype(jnp.float32), axis=1
    )
    features = jnp.transpose(summed.astype(jnp.bfloat16), (1, 0, 2)).reshape(
        dev_rows, n_tables * emb_width
    )
    samples = lax.all_gather(features, "section", axis=0, tiled=True)
    whole_weights = lax.all_gather(w_first, "dev", axis=0, tiled=True)
    pre_act = jnp.dot(samples, whole_weights, preferred_element_type=jnp.float32)
    hidden = jnp.maximum(pre_act + b_first.astype(jnp.float32)[None, :], 0.0)
    logit_part = jnp.sum(hidden * w_out.astype(jnp.float32)[None, :], axis=1)
    return lax.psum(logit_part, "section")


def solution(mesh):
    placed = (
        P(("section", "dev"), None, None),
        P(),
        P(("section", "dev"), None),
        P("dev", "section"),
        P("section"),
        P("section"),
    )
    return jax.shard_map(body, mesh=mesh, in_specs=placed, out_specs=P("dev"), check_vma=False)
```

```python
import functools

import jax
import jax.numpy as jnp
from jax import lax
from jax.experimental import pallas as pl
from jax.experimental.pallas import tpu as pltpu
from jax.sharding import PartitionSpec as P

VMEM_LIMIT = 60 * 1024 * 1024
RELAYED = (((3, 0),), ((3, 1), (2, 2)), ((3, 2),), ((2, 3), (3, 3)))


def bag_kernel(table_chunks, bags_per_step, pool_size, table_ref, ids_ref, out_ref, staged, wide, sums, sems):
    rows, _ = table_ref.shape
    chunk = rows // table_chunks

    def fetch(c):
        return pltpu.make_async_copy(table_ref.at[pl.ds(c * chunk, chunk)], staged.at[c % 2], sems.at[c % 2])

    fetch(0).start()
    wide[pl.ds(rows, 8), :] = jnp.zeros((8, wide.shape[1]), jnp.float32)
    for c in range(table_chunks):
        if c + 1 < table_chunks:
            fetch(c + 1).start()
        fetch(c).wait()
        step = 256

        def widen(k, carry):
            at = pl.multiple_of(k * step, step)
            wide[pl.ds(c * chunk + at, step), :] = staged[c % 2, pl.ds(at, step), :].astype(jnp.float32)
            return carry

        lax.fori_loop(0, chunk // step, widen, 0)

    def bags(r, carry):
        for b in range(bags_per_step):
            total = None
            for p in range(pool_size):
                row = wide[pl.ds(ids_ref[r, b * pool_size + p], 1), :]
                total = row if total is None else total + row
            sums[pl.ds(r * bags_per_step + b, 1), :] = total
        return carry

    lax.fori_loop(0, ids_ref.shape[0], bags, 0)
    out_ref[...] = sums[...].astype(jnp.bfloat16)


def pool_bags(table, ids, pool_size):
    rows, emb = table.shape
    bags_per_step = ids.shape[1] // pool_size
    n_bags = ids.shape[0] * bags_per_step
    chunks = 8
    return pl.pallas_call(
        functools.partial(bag_kernel, chunks, bags_per_step, pool_size),
        out_shape=jax.ShapeDtypeStruct((n_bags, emb), jnp.bfloat16),
        in_specs=[pl.BlockSpec(memory_space=pl.ANY), pl.BlockSpec(memory_space=pltpu.SMEM)],
        out_specs=pl.BlockSpec(memory_space=pltpu.VMEM),
        scratch_shapes=[
            pltpu.VMEM((2, rows // chunks, emb), jnp.bfloat16),
            pltpu.VMEM((rows + 8, emb), jnp.float32),
            pltpu.VMEM((n_bags, emb), jnp.float32),
            pltpu.SemaphoreType.DMA((2,)),
        ],
        compiler_params=pltpu.CompilerParams(vmem_limit_bytes=VMEM_LIMIT),
        cost_estimate=pl.CostEstimate(flops=n_bags * pool_size * emb * 600, bytes_accessed=rows * emb * 2, transcendentals=0),
        name="pool_bags",
    )(table, ids)


def step_kernel(
    secs, devs, pool_size,
    ids_ref, len_ref, table_ref, w_ref, b_ref, wo_ref, out_ref,
    ids_raw, ids_in, ids_safe, ids_smem, bias, project, staged, wide, sums, pooled, feats, weights, pre, outgoing, first_in, relay, second_in, mine, theirs,
    isend, irecv, icopy, scopy, vsem, tsem, fsend, ysend, dsend, frecv, wsend, wrecv, wlocal, asend, arecv, bsend, brecv, lsend, lrecv,
):
    rows, emb = table_ref.shape
    count = secs * devs
    per_dev, hid = w_ref.shape
    quarter = hid // 2
    chunks, samples, depth = feats.shape
    tiles = wsend.shape[1]
    tile = quarter // tiles
    width = quarter // asend.shape[1]
    pieces = tile // width
    bags_src = ids_ref.shape[2]
    sec, dev = lax.axis_index("section"), lax.axis_index("dev")
    me = sec * devs + dev
    z, y, x = dev // 4, lax.rem(dev // 2, 2), lax.rem(dev, 2)
    zh, zl = z // 2, lax.rem(z, 2)

    def device(position):
        return {"section": position // devs, "dev": lax.rem(position, devs)}

    def place(s, zz, yy, xx):
        return {"section": s, "dev": zz * 4 + yy * 2 + xx}

    table_chunks = 8
    piece = rows // table_chunks

    def fetch(c):
        return pltpu.make_async_copy(table_ref.at[pl.ds(c * piece, piece)], staged.at[c % 2], tsem.at[c % 2])

    barrier = pltpu.get_barrier_semaphore()
    for k in range(1, count):
        pl.semaphore_signal(barrier, inc=1, device_id=device(lax.rem(me + k, count)))

    raw_ids = pltpu.make_async_copy(ids_ref, ids_raw, icopy)
    raw_ids.start()
    small = [
        pltpu.make_async_copy(b_ref, bias, vsem.at[0]),
        pltpu.make_async_copy(wo_ref, project, vsem.at[1]),
    ]
    for copy in small:
        copy.start()
    fetch(0).start()
    own_slot = zl * 2 + y
    own_cols = pl.ds(pl.multiple_of(y * quarter, quarter), quarter)
    own_weights = pltpu.make_async_copy(w_ref.at[:, own_cols], weights.at[own_slot], wlocal)
    own_weights.start()
    raw_ids.wait()
    slot_row = lax.broadcasted_iota(jnp.int32, ids_ref.shape[1:], 0)
    for t in range(count):
        ids_safe[t] = jnp.where(slot_row < len_ref[t], ids_raw[t], rows)
    wide[pl.ds(rows, 8), :] = jnp.zeros((8, emb), jnp.float32)
    step = 256
    for c in range(table_chunks):
        if c + 1 < table_chunks:
            fetch(c + 1).start()
        fetch(c).wait()

        def widen(k, carry):
            at = pl.multiple_of(k * step, step)
            wide[pl.ds(c * piece + at, step), :] = staged[c % 2, pl.ds(at, step), :].astype(jnp.float32)
            return carry

        lax.fori_loop(0, piece // step, widen, 0)

    pl.semaphore_wait(barrier, count - 1)

    my_pair = me // 2
    my_zh, my_u, my_x, my_h = my_pair // 8, lax.rem(my_pair // 2, 4), lax.rem(my_pair, 2), lax.rem(me, 2)
    my_place = ids_in.at[my_zh, my_u, my_x, pl.ds(pl.multiple_of(my_h * pool_size, pool_size), pool_size)]

    for j in range(4):
        for i in range(8):
            to_sec = 1 - my_zh if j < 2 else my_zh
            to_y = 1 - my_x if j % 2 == 0 else my_x
            to_z = lax.rem(z + 2 + i // 2, 4)
            other = to_sec * devs + to_z * 4 + to_y * 2 + i % 2
            remote = pltpu.make_async_remote_copy(
                src_ref=ids_safe.at[other], dst_ref=my_place, send_sem=isend, recv_sem=irecv.at[j],
                device_id=device(other),
            )
            own_ids = pltpu.make_async_copy(ids_safe.at[me], my_place, irecv.at[j])

            @pl.when(other == me)
            def _():
                own_ids.start()

            @pl.when(other != me)
            def _():
                remote.start()

    started = []
    shipped = {}

    def ship(r, n):
        cols = pl.ds(n * tile, tile)
        if r == 1:
            source = w_ref.at[:, pl.ds(pl.multiple_of((1 - y) * quarter + n * tile, tile), tile)]
        elif r == 2:
            source = w_ref.at[:, pl.ds(pl.multiple_of(y * quarter + n * tile, tile), tile)]
        else:
            shipped[1, n].wait_recv()
            source = weights.at[zl * 2 + 1 - y, :, cols]
        slot = zl * 2 + 1 - y if r == 3 else own_slot
        copy = pltpu.make_async_remote_copy(
            src_ref=source, dst_ref=weights.at[slot, :, cols],
            send_sem=wsend.at[r - 1, n], recv_sem=wrecv.at[r - 1, n],
            device_id=place(sec, z, 1 - y, x) if r == 1 else place(sec, zh * 2 + 1 - zl, y, x),
        )
        copy.start()
        started.append(copy)
        shipped[r, n] = copy

    for n in range(tiles):
        ship(1, n)
        if n < 2:
            ship(2, n)

    def part_of(j, c):
        return feats.at[j, :, pl.ds(pl.multiple_of(c * emb, emb), emb)]

    def arrival(j, c):
        part = part_of(j, c)
        return pltpu.make_async_copy(part, part, frecv.at[j, c])

    def landed(j, c):
        part = part_of(j, c)
        pltpu.make_async_copy(part, part, frecv.at[j, c]).wait()
        return part

    def across(j, c, lane):
        part = part_of(j, c)
        return pltpu.make_async_remote_copy(
            src_ref=part, dst_ref=part, send_sem=dsend.at[j, lane], recv_sem=frecv.at[j, c],
            device_id=place(1 - sec, z, y, x),
        )

    def beside(j, c, lane):
        part = part_of(j, c)
        return pltpu.make_async_remote_copy(
            src_ref=part, dst_ref=part, send_sem=ysend.at[j, lane], recv_sem=frecv.at[j, c],
            device_id=place(sec, z, 1 - y, x),
        )

    kept = []
    shared = {}

    def begin(copy):
        copy.start()
        started.append(copy)

    def forward(j):
        if j < 2:
            for i in range(2):
                c = (sec + 2 * i) * 2 + lax.rem(y + j, 2)
                landed(j, c)
                begin(beside(j, c, i))
                begin(across(j, c, i))
            return
        columns = [(sec + 2 * i) * 2 + b for i in range(2) for b in range(2)]
        aside = [beside(j, c, lane) for lane, c in enumerate(columns)]
        shared[j] = [across(j, c, lane) for lane, c in enumerate(columns)]
        arrivals = [arrival(j, c) for c in columns]

        @pl.when(x == y)
        def _():
            for arrived, sideways, copy in zip(arrivals, aside, shared[j]):
                arrived.wait()
                sideways.start()
                copy.start()

        kept.extend((x != y, copy) for copy in aside)
        started.extend(shared[j])

    def share(j):
        if j < 2:
            for i in range(2):
                c = (sec + 2 * i) * 2 + lax.rem(y + j + 1, 2)
                landed(j, c)
                begin(across(j, c, 2 + i))
            return
        arrivals = [arrival(j, (sec + 2 * i) * 2 + b) for i in range(2) for b in range(2)]

        @pl.when(x != y)
        def _():
            for arrived, copy in zip(arrivals, shared[j]):
                arrived.wait()
                copy.start()

    def complete(j):
        for i in range(2):
            for b in range(2):
                landed(j, (1 - sec + 2 * i) * 2 + b)

    column = z * 2 + x
    def stage_ids(j):
        to_x = 1 - y if j % 2 == 0 else y
        to_zh = 1 - sec if j < 2 else sec
        ids_part = ids_in.at[to_zh, :, to_x]
        pltpu.make_async_copy(ids_part, ids_part, irecv.at[j]).wait()
        lines = [
            pltpu.make_async_copy(
                ids_part.at[u], ids_smem.at[j % 2, pl.ds(2 * pool_size * u, 2 * pool_size)], scopy.at[j % 2, u]
            )
            for u in range(4)
        ]
        for copy in lines:
            copy.start()
        return lines

    staged_ids = {0: stage_ids(0)}

    def pool(j, half):
        def bags(u, lines):
            for b in range(bags_src):
                total = None
                for p in range(pool_size):
                    row = wide[pl.ds(ids_smem[j % 2, lines[p], b], 1), :]
                    total = row if total is None else total + row
                sums[u, pl.ds(b, 1), :] = total
            return tuple(line + pool_size for line in lines)

        start = 4 * half
        lax.fori_loop(start, start + 4, bags, tuple(jnp.int32(start * pool_size + p) for p in range(pool_size)))
        pooled[j, half] = sums[start:start + 4].astype(jnp.bfloat16).reshape(samples, emb)
        dst = part_of(j, column)
        copy = pltpu.make_async_remote_copy(
            src_ref=pooled.at[j, half], dst_ref=dst, send_sem=fsend.at[j, half], recv_sem=frecv.at[j, column],
            device_id=place(lax.rem(z, 2), 2 * sec + half, lax.rem(x + j, 2) if j < 2 else y, y),
        )
        local = pltpu.make_async_copy(pooled.at[j, half], dst, frecv.at[j, column])
        keeps = jnp.logical_and(
            jnp.logical_and(lax.rem(z, 2) == sec, 2 * sec + half == z),
            jnp.logical_and(x == y, lax.rem(x + j, 2) == y) if j < 2 else x == y,
        )

        @pl.when(keeps)
        def _():
            local.start()

        @pl.when(jnp.logical_not(keeps))
        def _():
            copy.start()

        kept.append((keeps, copy))

    for j in range(chunks):
        for copy in staged_ids[j]:
            copy.wait()
        if j + 1 < chunks:
            staged_ids[j + 1] = stage_ids(j + 1)
        pool(j, 0)
        if j == 2:
            forward(0)
        pool(j, 1)
        if j == 2:
            forward(1)
        if j == 3:
            share(0)
        for r, n in RELAYED[j]:
            ship(r, n)

    own_weights.wait()
    first, second = {}, {}

    def multiply(j, n):
        cols = pl.ds(n * tile, tile)
        return jnp.dot(
            feats[j], weights[:, :, cols].reshape(depth, tile), preferred_element_type=jnp.float32
        )

    def give(b, n):
        cols = pl.ds(n * tile, tile)
        outgoing[b, :, cols] = multiply(2 * b, n).astype(jnp.bfloat16)
        for m in range(n * pieces, (n + 1) * pieces):
            cols = pl.ds(m * width, width)
            copy = pltpu.make_async_remote_copy(
                src_ref=outgoing.at[b, :, cols], dst_ref=first_in.at[b, :, cols],
                send_sem=asend.at[b, m], recv_sem=arecv.at[b, m], device_id=place(sec, z, y, 1 - x),
            )
            copy.start()
            started.append(copy)
            first[b, m] = copy

    def hand_on(n):
        for m in range(n * pieces, (n + 1) * pieces):
            cols = pl.ds(m * width, width)
            first[0, m].wait_recv()
            relay[:, cols] = (pre[0, :, cols] + first_in[0, :, cols].astype(jnp.float32)).astype(jnp.bfloat16)
            copy = pltpu.make_async_remote_copy(
                src_ref=relay.at[:, cols], dst_ref=second_in.at[:, cols],
                send_sem=bsend.at[m], recv_sem=brecv.at[m],
                device_id=place(sec, lax.rem(z + 2, 4), y, x),
            )
            copy.start()
            started.append(copy)
            second[m] = copy

    def keep(b, n):
        pre[b, :, pl.ds(n * tile, tile)] = multiply(2 * b + 1, n)

    def lead(n):
        for r in (2, 3):
            shipped[r, n].wait_recv()
        give(0, n)

    complete(0)
    lead(0)
    lead(1)
    share(1)
    forward(2)
    complete(1)
    keep(0, 0)
    hand_on(0)
    keep(0, 1)
    lead(2)
    hand_on(1)
    forward(3)
    share(2)
    lead(3)
    keep(0, 2)
    hand_on(2)
    keep(0, 3)
    complete(2)
    give(1, 0)
    hand_on(3)
    give(1, 1)
    give(1, 2)
    share(3)
    give(1, 3)
    complete(3)
    for n in range(tiles):
        keep(1, n)

    for copy in small:
        copy.wait()
    acc = jnp.zeros((samples, 128), jnp.float32)
    for m in range(quarter // width):
        cols, other = pl.ds(m * width, width), pl.ds(quarter + m * width, width)
        first[1, m].wait_recv()
        total = pre[1, :, cols] + first_in[1, :, cols].astype(jnp.float32)
        second[m].wait_recv()
        total = total + second_in[:, cols].astype(jnp.float32)
        shift = jnp.where(y == 0, bias[cols].astype(jnp.float32), bias[other].astype(jnp.float32))
        scale = jnp.where(y == 0, project[cols].astype(jnp.float32), project[other].astype(jnp.float32))
        hidden = jnp.maximum(total + shift[None, :], 0.0)
        weighed = hidden * scale[None, :]
        for q in range(width // 128):
            acc = acc + weighed[:, q * 128:(q + 1) * 128]
    logits = jnp.sum(acc.T, axis=0, keepdims=True)
    half = samples // 2
    for b in range(2):
        mine[b] = logits[:, b * half:(b + 1) * half]
    swaps = []
    for r in (1, 2, 3):
        to_y = 1 - y if r & 1 else y
        to_sec = 1 - sec if r & 2 else sec
        swap = pltpu.make_async_remote_copy(
            src_ref=mine.at[to_y], dst_ref=theirs.at[r - 1], send_sem=lsend.at[r - 1], recv_sem=lrecv.at[r - 1],
            device_id=place(to_sec, z, to_y, x),
        )
        swap.start()
        swaps.append(swap)
    for swap in swaps:
        swap.wait_recv()
    out_ref[...] = mine[y] + theirs[0] + theirs[1] + theirs[2]
    for copy in started + swaps:
        copy.wait_send()
    for keeps, copy in kept:

        @pl.when(jnp.logical_not(keeps))
        def _():
            copy.wait_send()

    sent = ids_safe.at[pl.ds(0, count - 1)]
    pltpu.make_async_copy(sent, sent, isend).wait()


def whole_step(secs, devs, pool_size, ids, pool_len, table, w_first, bias, w_out):
    rows, emb = table.shape
    per_dev, hid = w_first.shape
    quarter = hid // 2
    bags_src = ids.shape[2]
    samples = 4 * bags_src
    depth = 4 * per_dev
    tiles = 4
    parts = 8
    columns = depth // emb
    vm = pl.BlockSpec(memory_space=pltpu.VMEM)
    anywhere = pl.BlockSpec(memory_space=pl.ANY)
    dma = pltpu.SemaphoreType.DMA
    return pl.pallas_call(
        functools.partial(step_kernel, secs, devs, pool_size),
        out_shape=jax.ShapeDtypeStruct((1, samples // 2), jnp.float32),
        in_specs=[anywhere, pl.BlockSpec(memory_space=pltpu.SMEM), anywhere, anywhere, anywhere, anywhere],
        out_specs=vm,
        scratch_shapes=[
            pltpu.VMEM(ids.shape, jnp.int32),
            pltpu.VMEM((2, 4, 2, 2 * pool_size, bags_src), jnp.int32),
            pltpu.VMEM(ids.shape, jnp.int32),
            pltpu.SMEM((2, 8 * pool_size, bags_src), jnp.int32),
            pltpu.VMEM((hid,), jnp.bfloat16),
            pltpu.VMEM((hid,), jnp.bfloat16),
            pltpu.VMEM((2, rows // 8, emb), jnp.bfloat16),
            pltpu.VMEM((rows + 8, emb), jnp.float32),
            pltpu.VMEM((8, bags_src, emb), jnp.float32),
            pltpu.VMEM((4, 2, samples, emb), jnp.bfloat16),
            pltpu.VMEM((4, samples, depth), jnp.bfloat16),
            pltpu.VMEM((4, per_dev, quarter), jnp.bfloat16),
            pltpu.VMEM((2, samples, quarter), jnp.float32),
            pltpu.VMEM((2, samples, quarter), jnp.bfloat16),
            pltpu.VMEM((2, samples, quarter), jnp.bfloat16),
            pltpu.VMEM((samples, quarter), jnp.bfloat16),
            pltpu.VMEM((samples, quarter), jnp.bfloat16),
            pltpu.VMEM((2, 1, samples // 2), jnp.float32),
            pltpu.VMEM((3, 1, samples // 2), jnp.float32),
            dma, dma((4,)), dma, dma((2, 4)), dma((2,)), dma((2,)),
            dma((4, 2)), dma((4, 4)), dma((4, 4)), dma((4, columns)),
            dma((3, tiles)), dma((3, tiles)), dma,
            dma((2, parts)), dma((2, parts)), dma((parts,)), dma((parts,)),
            dma((3,)), dma((3,)),
        ],
        compiler_params=pltpu.CompilerParams(collective_id=0, has_side_effects=True, vmem_limit_bytes=VMEM_LIMIT),
        name="whole_step",
    )(ids, pool_len, table, w_first, bias, w_out)


def body(indices, pool_len, tables, w_first, b_first, w_out):
    sec_count = lax.axis_size("section")
    dev_count = lax.axis_size("dev")
    devices = sec_count * dev_count
    dev_rows, n_tables, pool_size = indices.shape
    rows_dev, emb_width = tables.shape
    row_split = devices // n_tables
    position = lax.axis_index("section") * dev_count + lax.axis_index("dev")
    table_id = position // row_split
    first_row = position % row_split * rows_dev
    square = row_split == 1 and sec_count == 2 and dev_count == 16
    if square and w_first.shape[0] == 2 * emb_width and w_first.shape[1] % 2048 == 0 and dev_rows % 64 == 0:
        ids = jnp.transpose(indices, (1, 2, 0))
        logits = whole_step(
            sec_count, dev_count, pool_size, ids, pool_len, tables, w_first, b_first, w_out
        )
        return logits.reshape(logits.shape[1])
    outgoing = jnp.transpose(indices, (1, 0, 2)).reshape(n_tables, dev_rows * pool_size)
    outgoing = jnp.repeat(outgoing, row_split, axis=0)
    arrived = lax.all_to_all(outgoing, ("section", "dev"), split_axis=0, concat_axis=0, tiled=True)
    all_rows = devices * dev_rows
    wanted = arrived.reshape(all_rows * pool_size // 128, 128) - first_row
    live_slots = jnp.sum(jnp.where(jnp.arange(n_tables) == table_id, pool_len, 0))
    slot = jnp.arange(128) % pool_size
    usable = (wanted >= 0) & (wanted < rows_dev) & (slot < live_slots)[None, :]
    safe_rows = jnp.where(usable, wanted, rows_dev)
    partial_value = pool_bags(tables, safe_rows, pool_size)
    ordered = jnp.transpose(
        partial_value.reshape(dev_count, sec_count, dev_rows, emb_width), (1, 0, 2, 3)
    )
    received = lax.all_to_all(
        ordered.reshape(devices, dev_rows, emb_width),
        ("section", "dev"),
        split_axis=0,
        concat_axis=0,
        tiled=True,
    )
    summed = jnp.sum(
        received.reshape(n_tables, row_split, dev_rows, emb_width).astype(jnp.float32), axis=1
    )
    features = jnp.transpose(summed.astype(jnp.bfloat16), (1, 0, 2)).reshape(
        dev_rows, n_tables * emb_width
    )
    samples = lax.all_gather(features, "section", axis=0, tiled=True)
    whole_weights = lax.all_gather(w_first, "dev", axis=0, tiled=True)
    pre_act = jnp.dot(samples, whole_weights, preferred_element_type=jnp.float32)
    hidden = jnp.maximum(pre_act + b_first.astype(jnp.float32)[None, :], 0.0)
    logit_part = jnp.sum(hidden * w_out.astype(jnp.float32)[None, :], axis=1)
    return lax.psum(logit_part, "section")


def solution(mesh):
    placed = (
        P(("section", "dev"), None, None),
        P(),
        P(("section", "dev"), None),
        P("dev", "section"),
        P("section"),
        P("section"),
    )
    return jax.shard_map(body, mesh=mesh, in_specs=placed, out_specs=P("dev"), check_vma=False)
```
